32 devices in a mesh: facet: 4 (over z), chan: 8 (over y, x, core).
Axes of the slice: x: 2, y: 2, z: 4, core: 2. Of those that a mesh axis runs over, the one named last changes fastest.
Arguments:
- visibilities: bfloat16 [2, 8, 256, 32, 128], P(None, None, None, ('facet', 'chan')), may hold values from -12 to 12
- kernels: bfloat16 [32, 256, 512], replicated, may hold values from -0.25 to 0.25
- delays: float32 [8, 256, 128], P('facet'), may hold values from -4 to 4
- tile_of: int32 [8, 256], P('facet'), may hold values from 0 to 127
- plane_of: int32 [8, 256], P('facet'), may hold values from 0 to 31
- counts: int32 [8], P('facet'), may hold values from 64 to 256
- neighbours: int32 [8, 4], replicated, may hold values from 0 to 7, as said below
Outputs:
- joined_grids: float32 [128, 8, 4, 512], P('chan', 'facet')
The draws below stay inside these ranges and needn't reach their ends.
Inputs may be any that keep to these rules, and one draw needn't show every extreme that they name: `neighbours`: each row names 4 different facets, none of them its own.
All inputs are finite; a program needn't handle non-finite values.
Results may differ from the reference program's by a relative error of at most 0.0043.
Values may be sent and summed in bfloat16 or wider, within the bound.
A program may use at most 128 MiB of HBM per device.

```python
import math
import jax
import jax.numpy as jnp
from jax import lax

FACETS = 8
BLOCKS = 256
CHANNELS = 32
AVG = 8
OUTCH = 4
BV = 128
TS = 16
TILE = 256
NTILES = 128
WPLANES = 32
EDGE = 4
NNB = 4


def draw_neighbours(key, part):
    facet_keys = jax.random.split(jax.random.fold_in(key, 7), FACETS)

    def draw_row(row_key, facet_id):
        shuffled = jax.random.permutation(row_key, FACETS - 1)[:NNB].astype(jnp.int32)
        return jnp.where(shuffled >= facet_id, shuffled + 1, shuffled).astype(jnp.int32)
    return jax.vmap(draw_row)(facet_keys, jnp.arange(FACETS, dtype=jnp.int32))


def plant(result, stream_key, smallest, largest):
    place = [jax.random.randint(jax.random.fold_in(stream_key, axis), (), 0, length) for axis, length in enumerate(result.shape)]
    widest = result.shape.index(max(result.shape))
    beside = place[:widest] + [(place[widest] + 1) % result.shape[widest]] + place[widest + 1:]
    return result.at[tuple(place)].set(smallest).at[tuple(beside)].set(largest)


def levels(key, dims, pieces, least, top_value):
    gain = 1.0
    for dim, blocks in pieces:
        heights = jax.random.uniform(jax.random.fold_in(jax.random.fold_in(key, 6), dim), (blocks,), jnp.float32, least / len(pieces), top_value / len(pieces))
        gain = gain * jnp.repeat(jnp.exp(heights), dims[dim] // blocks).reshape((-1,) + (1,) * (len(dims) - 1 - dim))
    return gain


def bell_draw(own_key, extent, spread, reach, pieces=(), kind=jnp.bfloat16):
    array = spread * jax.random.normal(own_key, extent, jnp.float32)
    if pieces:
        array = array * levels(own_key, extent, pieces, -0.22, 0.18)
    return jnp.clip(array, -reach, reach).astype(kind)


def setup_inputs(seed: int = 0) -> dict:
    arg_keys = jax.random.split(jax.random.key(seed), 8)
    return {
        "visibilities": bell_draw(arg_keys[0], (2, FACETS, BLOCKS, CHANNELS, BV), 2.0, 12.0, ((3, 32),)),
        "kernels": bell_draw(arg_keys[1], (WPLANES, 2 * BV, 2 * TILE), (2 * BV * BLOCKS // NTILES) ** -0.5, 0.25),
        "delays": jnp.clip(jax.random.uniform(arg_keys[2], (FACETS, BLOCKS, BV), jnp.float32, -4.0, 4.0) * levels(arg_keys[2], (FACETS, BLOCKS, BV), ((0, 4),), -0.4, 0.0), -4.0, 4.0),
        "tile_of": plant(jax.random.randint(arg_keys[3], (FACETS, BLOCKS), 0, NTILES), jax.random.fold_in(arg_keys[3], 1), 0, NTILES - 1).astype(jnp.int32),
        "plane_of": plant(jax.random.randint(arg_keys[4], (FACETS, BLOCKS), 0, WPLANES), jax.random.fold_in(arg_keys[4], 1), 0, WPLANES - 1).astype(jnp.int32),
        "counts": plant(jax.random.randint(arg_keys[5], (FACETS,), BLOCKS // 4, BLOCKS + 1), jax.random.fold_in(arg_keys[5], 1), BLOCKS // 4, BLOCKS).astype(jnp.int32),
        "neighbours": draw_neighbours(jax.random.fold_in(arg_keys[7], 71), 0),
    }


def reference(visibilities, kernels, delays, tile_of, plane_of, counts, neighbours):
    highest = lax.Precision.HIGHEST
    channel = jnp.arange(CHANNELS, dtype=jnp.float32)
    freq_turn = (2.0 * math.pi) * (1.0 + 0.5 * channel / CHANNELS)
    group_rows = math.gcd(BLOCKS, 64)

    def grid_facet(facet_id):
        vis_facet = lax.dynamic_index_in_dim(visibilities, facet_id, 1, keepdims=False)
        delay_facet = lax.dynamic_index_in_dim(delays, facet_id, 0, keepdims=False)
        tiles_facet = lax.dynamic_index_in_dim(tile_of, facet_id, 0, keepdims=False)
        planes_facet = lax.dynamic_index_in_dim(plane_of, facet_id, 0, keepdims=False)
        live_count = lax.dynamic_index_in_dim(counts, facet_id, 0, keepdims=False)

        def one_group(grid_acc, group_index):
            begin_row = (group_index * group_rows).astype(jnp.int32)
            vis_piece = lax.dynamic_slice_in_dim(vis_facet, begin_row, group_rows, 1).astype(jnp.float32)
            delay_piece = lax.dynamic_slice_in_dim(delay_facet, begin_row, group_rows, 0)
            phase_angle = delay_piece[:, None, :] * freq_turn[None, :, None]
            cosine = jnp.cos(phase_angle)
            sine_part = jnp.sin(phase_angle)
            rot_real = vis_piece[0] * cosine - vis_piece[1] * sine_part
            rot_imag = vis_piece[0] * sine_part + vis_piece[1] * cosine
            avg_real = jnp.mean(rot_real.reshape(group_rows, OUTCH, AVG, BV), axis=2)
            avg_imag = jnp.mean(rot_imag.reshape(group_rows, OUTCH, AVG, BV), axis=2)
            avg_rows = jnp.concatenate([avg_real, avg_imag], axis=-1).astype(jnp.bfloat16)
            plane_piece = lax.dynamic_slice_in_dim(planes_facet, begin_row, group_rows, 0).astype(jnp.int32)
            chosen = jnp.take(kernels, plane_piece, axis=0)
            contrib = jnp.einsum("gcv,gvx->gcx", avg_rows.astype(jnp.float32), chosen.astype(jnp.float32), precision=highest)
            block_ids = begin_row + jnp.arange(group_rows, dtype=jnp.int32)
            live_mask = (block_ids < live_count).astype(jnp.float32)
            tile_piece = lax.dynamic_slice_in_dim(tiles_facet, begin_row, group_rows, 0).astype(jnp.int32)
            grid_acc = grid_acc.at[tile_piece].add(contrib * live_mask[:, None, None])
            return grid_acc, None

        start_grid = jnp.zeros((NTILES, OUTCH, 2 * TILE), jnp.float32)
        grid_acc, unused = lax.scan(one_group, start_grid, jnp.arange(BLOCKS // group_rows, dtype=jnp.int32))
        return grid_acc

    facet_grids = lax.map(grid_facet, jnp.arange(FACETS, dtype=jnp.int32))
    facet_grids = jnp.transpose(facet_grids, (1, 0, 2, 3))
    edge_cells = EDGE * TS
    strips = jnp.concatenate([facet_grids[..., :edge_cells], facet_grids[..., TILE:TILE + edge_cells]], axis=-1)
    neighbour_strips = jnp.take(strips, neighbours.astype(jnp.int32), axis=1)
    blended = 0.25 * jnp.sum(neighbour_strips, axis=2)
    joined = facet_grids.at[..., TILE - edge_cells:TILE].add(blended[..., :edge_cells])
    joined = joined.at[..., 2 * TILE - edge_cells:].add(blended[..., edge_cells:])
    return joined
```

```python
import functools
import math

import jax
import jax.numpy as jnp
from jax import lax
from jax.experimental import pallas as pl
from jax.experimental.pallas import tpu as pltpu
from jax.sharding import PartitionSpec as P

AVG = 8
TS = 16
NT_DEV = 16
EDGE = 4
LANES = 128
JOINED = 3
ORDER = (3, 0, 1, 2)
FIRST = 2
MESH = pl.DeviceIdType.MESH


def series(first, count, scale):
    return [
        (-1.0) ** i * scale ** (2 * i + first) / math.factorial(2 * i + first)
        for i in range(count)
    ]


SIN_HALF = series(1, 7, math.pi)
COS_HALF = series(0, 7, math.pi)


def turn_parts(turns):
    frac = turns - jnp.round(turns)
    square = frac * frac
    sine = jnp.full_like(frac, SIN_HALF[-1])
    cosine = jnp.full_like(frac, COS_HALF[-1])
    for a, b in zip(SIN_HALF[-2::-1], COS_HALF[-2::-1]):
        sine = sine * square + a
        cosine = cosine * square + b
    sine = sine * frac
    return 1.0 - 2.0 * sine * sine, 2.0 * sine * cosine


def flip(index, mask):
    bit = 1
    while bit <= mask:
        if mask & bit:
            index = index + bit - 2 * bit * lax.rem(index // bit, 2)
        bit *= 2
    return index


def kernel(
    cfg,
    neigh_hbm,
    count_hbm,
    vis_ref,
    delay_ref,
    tile_hbm,
    plane_hbm,
    kern_ref,
    out_ref,
    neigh_ref,
    count_ref,
    tile_ref,
    plane_ref,
    pair,
    part,
    got,
    raw,
    wide,
    rough,
    low,
    turns,
    codes,
    rows,
    kern,
    lhs,
    grid,
    final,
    mate_send,
    mate_recv,
    rough_send,
    rough_recv,
    low_send,
    low_recv,
    turn_send,
    turn_recv,
    code_send,
    code_recv,
    part_send,
    part_recv,
    raw_send,
    raw_recv,
    row_send,
    row_recv,
    relay_send,
    relay_recv,
    fin_send,
    fin_recv,
    own_sem,
    small_sem,
):
    n, nz, facets, fac, blk, groups, planes, tiles, joined, order = cfg
    me = lax.axis_index("chan")
    zme = lax.axis_index("facet")
    channels = groups * AVG * nz
    tile = kern_ref.shape[1] // 2
    edge = EDGE * TS
    pairs = n // 2
    parity = lax.rem(me, 2)
    mate = me + 1 - 2 * parity
    my_pair = me // 2
    half_avg = AVG // 2
    blocks = blk * n
    chunk_z = [flip(zme, c) for c in range(nz)]
    far_first = list(range(nz - 1, 0, -1))

    def group_of(c):
        return pl.ds(chunk_z[c] * fac, fac)

    barrier = pltpu.get_barrier_semaphore()
    for d in range(1, n):
        pl.semaphore_signal(
            barrier, inc=1, device_id={"chan": lax.rem(me + d, n)}, device_id_type=MESH
        )
    for d in range(1, nz):
        pl.semaphore_signal(
            barrier, inc=1, device_id={"facet": chunk_z[d]}, device_id_type=MESH
        )

    def local_copy(src, dst, sem):
        return pltpu.make_async_copy(src, dst, sem)

    own_wide = local_copy(delay_ref.at[:, :, parity], wide, small_sem.at[0])
    small = [
        local_copy(tile_hbm, tile_ref, small_sem.at[1]),
        local_copy(plane_hbm, plane_ref, small_sem.at[2]),
        local_copy(count_hbm, count_ref, small_sem.at[3]),
        local_copy(neigh_hbm, neigh_ref, small_sem.at[4]),
    ]
    load_kern = local_copy(kern_ref, kern, small_sem.at[5])

    def own_copy(c):
        if c >= joined:
            return local_copy(
                vis_ref.at[:, group_of(c), my_pair, parity], raw.at[me, c - joined], own_sem.at[c]
            )
        return local_copy(
            vis_ref.at[:, group_of(c), :, parity], pair.at[parity, c], own_sem.at[c]
        )

    def chan_copy(src, dst, send, recv, peer):
        return pltpu.make_async_remote_copy(
            src_ref=src,
            dst_ref=dst,
            send_sem=send,
            recv_sem=recv,
            device_id={"chan": peer},
            device_id_type=MESH,
        )

    def facet_copy(src, dst, send, recv, c):
        return pltpu.make_async_remote_copy(
            src_ref=src,
            dst_ref=dst,
            send_sem=send,
            recv_sem=recv,
            device_id={"facet": chunk_z[c]},
            device_id_type=MESH,
        )

    own_wide.start()
    for copy in small:
        copy.start()
    for c in range(nz):
        own_copy(c).start()
    with jax.named_scope("barrier"):
        pl.semaphore_wait(barrier, n + nz - 2)

    def mate_copy(c, slot):
        return chan_copy(
            vis_ref.at[:, group_of(c), :, 1 - parity],
            pair.at[slot, c],
            mate_send,
            mate_recv.at[c],
            mate,
        )

    for c in range(joined):
        mate_copy(c, parity).start()
    for c in range(joined, nz):
        for m in range(n - 1, 0, -1):
            peer = flip(me, m)
            chan_copy(
                vis_ref.at[:, group_of(c), peer // 2, lax.rem(peer, 2)],
                raw.at[me, c - joined],
                raw_send,
                raw_recv.at[c - joined],
                peer,
            ).start()

    def rough_copy(c):
        return facet_copy(rough.at[0], rough.at[c], rough_send, rough_recv.at[c], c)

    def low_copy(c):
        return facet_copy(low.at[0], low.at[c], low_send, low_recv.at[c], c)

    def turn_copy(c):
        return facet_copy(
            wide.at[:, my_pair],
            turns.at[c - joined],
            turn_send,
            turn_recv.at[c - joined],
            c,
        )

    def code_copy(c):
        return facet_copy(codes.at[0], codes.at[c], code_send, code_recv.at[c], c)

    with jax.named_scope("delays"):
        own_wide.wait()
        rough[0] = wide[...].astype(jnp.bfloat16)
        for c in range(1, joined):
            rough_copy(c).start()
        mine = wide[:, my_pair]
        low[0] = (mine - mine.astype(jnp.bfloat16).astype(jnp.float32)).astype(jnp.bfloat16)
        for c in far_first:
            if c >= joined:
                turn_copy(c).start()
            else:
                low_copy(c).start()
    with jax.named_scope("codes"):
        for copy in small:
            copy.wait()
        block_id = lax.broadcasted_iota(jnp.int32, (1, blocks), 1)
        for i in range(fac):
            codes[0, i : i + 1] = jnp.where(
                block_id < count_ref[i],
                plane_ref[i : i + 1] * tiles + tile_ref[i : i + 1],
                -1,
            )
        for c in far_first:
            code_copy(c).start()

    def part_copy(c, peer, slot):
        return chan_copy(
            part.at[peer, c], got.at[slot, c], part_send, part_recv.at[c], 2 * peer + parity
        )

    def row_copy(c, peer):
        piece = rows.at[c, :, my_pair, parity]
        return chan_copy(piece, piece, row_send, row_recv.at[c], 2 * peer + parity)

    def relay_copy(c, side):
        piece = rows.at[c, :, :, side]
        return chan_copy(piece, piece, relay_send, relay_recv.at[c], mate)

    def join_pair(c):
        if c >= joined:
            return
        own_copy(c).wait()
        mate_copy(c, 1 - parity).wait_recv()
        if c:
            rough_copy(c).wait_recv()

        def one(i, carry):
            slot = i // pairs
            q = lax.rem(i, pairs)
            delay = rough[c, slot, q].astype(jnp.float32) if c else wide[slot, q]
            cosine, sine = turn_parts(delay * (0.5 / channels))
            real = pair[1, c, 0, slot, q].astype(jnp.float32)
            imag = pair[1, c, 1, slot, q].astype(jnp.float32)
            part[q, c, 0, slot] = (
                pair[0, c, 0, slot, q].astype(jnp.float32) + (real * cosine - imag * sine)
            ).astype(jnp.bfloat16)
            part[q, c, 1, slot] = (
                pair[0, c, 1, slot, q].astype(jnp.float32) + (real * sine + imag * cosine)
            ).astype(jnp.bfloat16)
            return carry

        lax.fori_loop(0, fac * pairs, one, 0)
        for m in range(pairs - 1, 0, -1):
            part_copy(c, flip(my_pair, m), my_pair).start()
        got[my_pair, c] = part[my_pair, c]

    def rotate(c):
        if c >= joined:
            turn_copy(c).wait_recv()
            own_copy(c).wait()
            every = raw.at[0 : n - 1, c - joined]
            chan_copy(every, every, raw_send, raw_recv.at[c - joined], mate).wait_recv()
            terms = AVG
        else:
            if c:
                low_copy(c).wait_recv()
            every = got.at[0 : pairs - 1, c]
            chan_copy(every, every, part_send, part_recv.at[c], mate).wait_recv()
            terms = half_avg
        step_turns = 0.5 * AVG / (terms * channels)

        def one(i, carry):
            if c >= joined:
                delay = turns[c - joined, i]
            elif c:
                delay = rough[c, i, my_pair].astype(jnp.float32) + low[c, i].astype(jnp.float32)
            else:
                delay = wide[i, my_pair]

            def term(k, p):
                block = raw[k, c - joined, p, i] if c >= joined else got[k, c, p, i]
                return block.astype(jnp.float32)

            step_cos, step_sin = turn_parts(delay * step_turns)
            for g in range(groups):
                first = (zme * groups + g) * AVG
                start_cos, start_sin = turn_parts(
                    delay * (1.0 + (0.5 / channels) * first.astype(jnp.float32))
                )
                top = (g + 1) * terms - 1
                real = term(top, 0)
                imag = term(top, 1)
                for k in range(top - 1, g * terms - 1, -1):
                    next_real = term(k, 0) + (real * step_cos - imag * step_sin)
                    imag = term(k, 1) + (real * step_sin + imag * step_cos)
                    real = next_real
                rows[c, i, my_pair, parity, :, 2 * LANES * g : 2 * LANES * g + LANES] = (
                    (real * start_cos - imag * start_sin) * (1.0 / AVG)
                ).astype(jnp.bfloat16)
                rows[c, i, my_pair, parity, :, 2 * LANES * g + LANES : 2 * LANES * (g + 1)] = (
                    (real * start_sin + imag * start_cos) * (1.0 / AVG)
                ).astype(jnp.bfloat16)
            return carry

        lax.fori_loop(0, fac, one, 0)
        for m in range(pairs - 1, 0, -1):
            row_copy(c, flip(my_pair, m)).start()

    def relay(c):
        every = rows.at[c, :, 0 : pairs - 1, 0]
        chan_copy(every, every, row_send, row_recv.at[c], mate).wait_recv()
        relay_copy(c, parity).start()

    entry = lax.broadcasted_iota(jnp.int32, (planes * NT_DEV, blocks), 0)
    wanted = (entry // NT_DEV) * tiles + me * NT_DEV + lax.rem(entry, NT_DEV)
    per_chunk = groups * fac * NT_DEV

    def gather_rows(c):
        if c:
            code_copy(c).wait_recv()
        relay_copy(c, 1 - parity).wait_recv()
        for i in range(fac):
            code = codes[c, i : i + 1]
            table = (code == wanted).astype(jnp.float32).astype(jnp.bfloat16)
            values = rows[c, i].reshape(blocks, rows.shape[-1])
            summed = jnp.dot(table, values, preferred_element_type=jnp.float32).astype(
                jnp.bfloat16
            )
            for g in range(groups):
                at = order.index(c) * per_chunk + (g * fac + i) * NT_DEV
                for p in range(planes):
                    lhs[at : at + NT_DEV, 2 * LANES * p : 2 * LANES * (p + 1)] = summed[
                        p * NT_DEV : (p + 1) * NT_DEV, 2 * LANES * g : 2 * LANES * (g + 1)
                    ]

    def fin_copy(c, first, width):
        columns = pl.ds(first, width)
        return facet_copy(
            final.at[c, :, :, columns], out_ref.at[zme, :, :, columns], fin_send, fin_recv, c
        )

    def put(c, first, width):
        at = order.index(c) * per_chunk
        for g in range(groups):
            here = at + g * fac * NT_DEV
            final[c, g, :, first : first + width] = grid[
                here : here + fac * NT_DEV, first : first + width
            ].astype(jnp.bfloat16)

    def multiply(top, bottom, first, width):
        grid[top:bottom, first : first + width] = jnp.dot(
            lhs[top:bottom],
            kern[:, first : first + width],
            preferred_element_type=jnp.float32,
        )

    span = nz * per_chunk
    early = FIRST * per_chunk

    def mm_first():
        load_kern.wait()
        multiply(0, early, 0, 2 * tile)
        for half in range(2):
            for c in far_first:
                if order.index(c) < FIRST:
                    put(c, half * tile, tile - LANES)
                    fin_copy(c, half * tile, tile - LANES).start()

    def blend_weights():
        row_id = lax.broadcasted_iota(jnp.int32, (NT_DEV, span), 0)
        col_id = lax.broadcasted_iota(jnp.int32, (NT_DEV, span), 1)
        same_tile = lax.rem(col_id, NT_DEV) == row_id
        slot = col_id // NT_DEV
        weights = []
        for c in order:
            for g in range(groups):
                for i in range(fac):
                    f = chunk_z[c] * fac + i
                    weight = jnp.zeros((NT_DEV, span), jnp.float32)
                    for k in range(neigh_ref.shape[0]):
                        other = neigh_ref[k, f]
                        there = jnp.zeros((NT_DEV, span), jnp.bool_)
                        for pos, b in enumerate(order):
                            base = (pos * groups + g) * fac
                            inside = (slot >= base) & (slot < base + fac)
                            there = there | (
                                inside & (slot - base + chunk_z[b] * fac == other)
                            )
                        weight += jnp.where(there & same_tile, 0.25, 0.0)
                    weights.append(weight)
        return jnp.concatenate(weights, axis=0).astype(jnp.bfloat16)

    keep = lax.broadcasted_iota(jnp.int32, (span, LANES), 1) >= LANES - edge

    runs = {
        "join": join_pair,
        "rotate": rotate,
        "relay": relay,
        "gather": gather_rows,
    }
    if nz == len(ORDER):
        plan = [
            ("join", 0),
            ("join", 1),
            ("join", 2),
            ("kern", 0),
            ("rotate", 3),
            ("rotate", 0),
            ("relay", 3),
            ("rotate", 1),
            ("relay", 0),
            ("gather", 3),
            ("rotate", 2),
            ("relay", 1),
            ("gather", 0),
            ("first", 0),
            ("relay", 2),
            ("gather", 1),
            ("gather", 2),
        ]
    else:
        plan = [(what, c) for what in ("join", "rotate", "relay") for c in order]
        plan += [("kern", 0)]
        plan += [("gather", c) for c in order]
        plan += [("first", 0)]
    for what, c in plan:
        with jax.named_scope(what + str(c)):
            if what == "kern":
                load_kern.start()
            elif what == "first":
                mm_first()
            else:
                runs[what](c)

    with jax.named_scope("weights"):
        mix = blend_weights()
    for half in range(2):
        left = half * tile
        with jax.named_scope("mm" + str(half)):
            multiply(early, span, left, tile)
        with jax.named_scope("blend" + str(half)):
            blended = jnp.dot(
                mix,
                grid[:, left : left + LANES].astype(jnp.bfloat16),
                preferred_element_type=jnp.float32,
            )
            moved = pltpu.roll(blended, LANES - edge, 1)
            grid[:, left + tile - LANES : left + tile] += jnp.where(keep, moved, 0.0)
            for c in far_first + [0]:
                begun = c and order.index(c) < FIRST
                first = left + tile - LANES if begun else left
                width = LANES if begun else tile
                put(c, first, width)
                if c:
                    fin_copy(c, first, width).start()

    own_out = local_copy(final.at[0], out_ref.at[zme], small_sem.at[6])
    own_out.start()
    with jax.named_scope("drain"):
        def sent(ref, sem):
            chan_copy(ref, ref, sem, sem, mate).wait_send()

        sent(pair.at[0, 0:joined], mate_send)
        sent(part.at[0 : pairs - 1, 0:joined], part_send)
        if joined < nz:
            sent(raw.at[0 : n - 1], raw_send)
            sent(turns, turn_send)
        sent(rows.at[:, :, 0 : pairs - 1, 0], row_send)
        sent(rows.at[:, :, :, 0], relay_send)
        if joined > 1:
            sent(rough.at[1:joined], rough_send)
            sent(low.at[1:joined], low_send)
        sent(codes.at[1:nz], code_send)
        sent(final.at[1:nz], fin_send)
    with jax.named_scope("finwait"):
        every = out_ref.at[0 : nz - 1]
        chan_copy(every, every, fin_send, fin_recv, mate).wait_recv()
    own_out.wait()


def local(visibilities, kernels, delays, tile_of, plane_of, counts, neighbours):
    n = lax.axis_size("chan")
    nz = lax.axis_size("facet")
    halves, facets, blocks, ch_dev, lanes = visibilities.shape
    planes, depth, cells = kernels.shape
    fac = facets // nz
    blk = blocks // n
    pairs = n // 2
    groups = n * ch_dev // AVG
    tiles = NT_DEV * n
    vis = visibilities.reshape(halves, facets, pairs, 2, blk, lanes)
    joined = min(JOINED, nz)
    order = ORDER if nz == len(ORDER) else tuple(range(nz))
    cfg = (n, nz, facets, fac, blk, groups, planes, tiles, joined, order)
    dma = pltpu.SemaphoreType.DMA
    raws = max(nz - joined, 1)
    span = groups * facets * NT_DEV
    anywhere = pl.BlockSpec(memory_space=pl.ANY)
    out = pl.pallas_call(
        functools.partial(kernel, cfg),
        out_shape=jax.ShapeDtypeStruct((nz, groups, fac * NT_DEV, cells), jnp.bfloat16),
        in_specs=[anywhere] * 7,
        out_specs=anywhere,
        scratch_shapes=[
            pltpu.SMEM((neighbours.shape[1], facets), jnp.int32),
            pltpu.SMEM((fac,), jnp.int32),
            pltpu.VMEM((fac, blocks), jnp.int32),
            pltpu.VMEM((fac, blocks), jnp.int32),
            pltpu.VMEM((2, joined, halves, fac, pairs, blk, lanes), jnp.bfloat16),
            pltpu.VMEM((pairs, joined, halves, fac, blk, lanes), jnp.bfloat16),
            pltpu.VMEM((pairs, joined, halves, fac, blk, lanes), jnp.bfloat16),
            pltpu.VMEM((n, raws, halves, fac, blk, lanes), jnp.bfloat16),
            pltpu.VMEM((fac, pairs, blk, lanes), jnp.float32),
            pltpu.VMEM((joined, fac, pairs, blk, lanes), jnp.bfloat16),
            pltpu.VMEM((joined, fac, blk, lanes), jnp.bfloat16),
            pltpu.VMEM((raws, fac, blk, lanes), jnp.float32),
            pltpu.VMEM((nz, fac, blocks), jnp.int32),
            pltpu.VMEM((nz, fac, pairs, 2, blk, groups * depth), jnp.bfloat16),
            pltpu.VMEM((planes * depth, cells), jnp.bfloat16),
            pltpu.VMEM((span, planes * depth), jnp.bfloat16),
            pltpu.VMEM((span, cells), jnp.float32),
            pltpu.VMEM((nz, groups, fac * NT_DEV, cells), jnp.bfloat16),
            dma,
            dma((joined,)),
            dma,
            dma((joined,)),
            dma,
            dma((joined,)),
            dma,
            dma((raws,)),
            dma,
            dma((nz,)),
            dma,
            dma((joined,)),
            dma,
            dma((raws,)),
            dma,
            dma((nz,)),
            dma,
            dma((nz,)),
            dma,
            dma,
            dma((nz,)),
            dma((7,)),
        ],
        compiler_params=pltpu.CompilerParams(
            collective_id=0, has_side_effects=True, vmem_limit_bytes=60 * 1024 * 1024
        ),
    )(
        neighbours.T,
        counts,
        vis,
        delays.reshape(fac, pairs, 2, blk, lanes),
        tile_of,
        plane_of,
        kernels.reshape(planes * depth, cells),
    )
    spread = out.reshape(nz * groups, fac, NT_DEV, cells).astype(jnp.float32)
    return jnp.transpose(spread, (2, 1, 0, 3))


def solution(mesh):
    return jax.shard_map(
        local,
        mesh=mesh,
        in_specs=(
            P(None, None, None, ("facet", "chan"), None),
            P(),
            P("facet", None, None),
            P("facet", None),
            P("facet", None),
            P("facet"),
            P(),
        ),
        out_specs=P("chan", "facet", None, None),
        check_vma=False,
    )
```
